32 devices in a mesh: seq: 8 (over y, x, core), tp: 4 (over z).
Axes of the slice: x: 2, y: 2, z: 4, core: 2. Of those that a mesh axis runs over, the one named last changes fastest.
Arguments:
- x_old: bfloat16 [4096, 4608], P('seq', 'tp'), may hold values from -6 to 6
- old_blocks: int32 [8], replicated, may hold values from 1 to 4, 16 in all
- new_blocks: int32 [8], replicated, may hold values from 1 to 4, 16 in all
- order: int32 [8], replicated, may hold values from 0 to 7, as said below
- pre_gain: float32 [4608], replicated, may hold values from 0.25 to 1.75
- post_gain: float32 [4608], replicated, may hold values from 0.25 to 1.75
- w_query: bfloat16 [4608, 4096], P('seq', 'tp'), may hold values from -0.59765625 to 0.59765625
- w_key: bfloat16 [4608, 2048], P('seq', 'tp'), may hold values from -0.09375 to 0.09375
- w_value: bfloat16 [4608, 2048], P('seq', 'tp'), may hold values from -0.09375 to 0.09375
- w_out_t: bfloat16 [4608, 4096], P('seq', 'tp'), may hold values from -0.09375 to 0.09375
Outputs:
- layer_out: bfloat16 [4096, 4608], P(('seq', 'tp'))
The draws below stay inside these ranges and needn't reach their ends.
Inputs may be any that keep to these rules, and one draw needn't show every extreme that they name: `old_blocks`: counts of 128-row blocks, at least one each; they sum to 16, and the largest is exactly 4. `new_blocks`: counts of 128-row blocks, at least one each; they sum to 16, and the largest is exactly 4. A permutation of the seq indices with order[7] = 0 and order[3] = 7; the other indices, taken in increasing order, hold 1 to 6 in increasing order, except that aligned pairs of them (first and second, third and fourth, and so on) are swapped or not, pair by pair.
All inputs are finite; a program needn't handle non-finite values.
Results may differ from the reference program's by a relative error of at most 0.013.
Values may be sent and summed in bfloat16 or wider, within the bound.
A program may use at most 128 MiB of HBM per device.

```python
import math
import jax
import jax.numpy as jnp
import numpy as np
from jax import lax

D = 4608
HEADS = 32
KV_HEADS = 16
HEAD = 128
BLOCK = 128
CAP = 512
TOKENS = 2048
SLOTS = 4096
N_SEQ = 8
N_TP = 4


def draw_order(key, part):
    middle = N_SEQ - 2
    kept = [place for place in range(N_SEQ) if place != N_SEQ - 1 and place != N_SEQ // 2 - 1]
    flips = jax.random.randint(jax.random.fold_in(key, 7), (middle // 2,), 0, 2).astype(jnp.int32)
    ranks = jnp.arange(middle, dtype=jnp.int32)
    shards = (jnp.bitwise_xor(ranks, jnp.repeat(flips, 2)) + 1).astype(jnp.int32)
    result = jnp.zeros((N_SEQ,), jnp.int32)
    result = result.at[jnp.array(kept, dtype=jnp.int32)].set(shards)
    result = result.at[N_SEQ - 1].set(0)
    result = result.at[N_SEQ // 2 - 1].set(N_SEQ - 1)
    return result.astype(jnp.int32)


def block_levels(rng, shape, cuts, least, largest):
    factor_of = 1.0
    for axis_at, shards_of in cuts:
        steps = jax.random.uniform(jax.random.fold_in(jax.random.fold_in(rng, 6), axis_at), (shards_of,), jnp.float32, least / len(cuts), largest / len(cuts))
        factor_of = factor_of * jnp.repeat(jnp.exp(steps), shape[axis_at] // shards_of).reshape((-1,) + (1,) * (len(shape) - 1 - axis_at))
    return factor_of


def split_up(number_of, total, reach, slope):
    portions = [(1 << 20) // math.isqrt(standing ** slope) + 1 for standing in range(2, number_of + 1)]
    rest, holding = total - reach - (number_of - 1), [1] * (number_of - 1)
    while rest > 0:
        movable = [i for i in range(number_of - 1) if holding[i] < reach]
        pool, left = sum([portions[i] for i in movable]), rest
        for i in movable:
            addition = min(reach - holding[i], max(1, left * portions[i] // pool), rest)
            holding[i] = holding[i] + addition
            rest = rest - addition
    return np.array([reach] + holding)


def uneven_parts(rng, number_of, total, reach, skew):
    if number_of == 2:
        one = jax.random.randint(rng, (), max(1, total - reach), min(reach, total - 1) + 1)
        return jnp.stack([one, total - one])
    lengths = jnp.asarray(split_up(number_of, total, reach, skew), jnp.int32)
    twos = (number_of - 1) // 2
    donor, receiver = lengths[1:1 + 2 * twos:2], lengths[2:2 + 2 * twos:2]
    room = jnp.minimum(donor - 1, reach - receiver)
    shifted = jax.random.randint(jax.random.fold_in(rng, 1), (twos,), 0, 1 << 20) % (room + 1)
    lengths = lengths.at[1:1 + 2 * twos:2].set(donor - shifted).at[2:2 + 2 * twos:2].set(receiver + shifted)
    return lengths[jax.random.permutation(jax.random.fold_in(rng, 2), number_of)]


def noise(key, shape, scale, bound, pieces=(), kind=jnp.bfloat16):
    values = jax.random.normal(key, shape, jnp.float32) * scale
    if len(pieces) > 0:
        values = block_levels(key, shape, pieces, -0.22, 0.18) * values
    return jnp.clip(values, min=-bound, max=bound).astype(kind)


def setup_inputs(seed: int = 0) -> dict:
    key_list = jax.random.split(jax.random.key(seed), 11)
    return {
        "x_old": noise(key_list[0], (SLOTS, D), 1.0, 6.0, ((0, 8), (1, 4))),
        "old_blocks": uneven_parts(key_list[1], N_SEQ, TOKENS // BLOCK, CAP // BLOCK, 1).astype(jnp.int32),
        "new_blocks": uneven_parts(key_list[2], N_SEQ, TOKENS // BLOCK, CAP // BLOCK, 2).astype(jnp.int32),
        "order": draw_order(jax.random.fold_in(key_list[10], 71), 0),
        "pre_gain": jnp.clip(1.0 + 0.15 * jax.random.normal(key_list[4], (D,), jnp.float32), 0.25, 1.75),
        "post_gain": jnp.clip(1.0 + 0.15 * jax.random.normal(key_list[5], (D,), jnp.float32), 0.25, 1.75),
        "w_query": noise(key_list[6], (D, HEADS * HEAD), 0.1, 0.59765625, ((0, 8), (1, 4))),
        "w_key": noise(key_list[7], (D, KV_HEADS * HEAD), D ** -0.5, 0.09375, ((0, 8), (1, 4))),
        "w_value": noise(key_list[8], (D, KV_HEADS * HEAD), D ** -0.5, 0.09375, ((0, 8), (1, 4))),
        "w_out_t": noise(key_list[9], (D, HEADS * HEAD), (HEADS * HEAD) ** -0.5, 0.09375, ((0, 8), (1, 4))),
    }


EPS = 1e-06

def offsets(blocks):
    return ((jnp.cumsum(blocks) - blocks) * BLOCK).astype(jnp.int32)

def rotate(values, places):
    half = values.shape[-1] // 2
    inverse = jnp.exp(jnp.arange(half, dtype=jnp.float32) * (-2.0 * math.log(10000.0) / values.shape[-1]))
    angles = places.astype(jnp.float32)[:, None] * inverse[None, :]
    cosine = jnp.cos(angles)[:, None, :]
    sine = jnp.sin(angles)[:, None, :]
    first = values[..., :half]
    second = values[..., half:]
    return jnp.concatenate([first * cosine - second * sine, second * cosine + first * sine], axis=-1)

def rms_scale(values, gain):
    return values * lax.rsqrt(lax.optimization_barrier(jnp.mean(values * values, axis=-1, keepdims=True)) + EPS) * gain

def reference(x_old, old_blocks, new_blocks, order, pre_gain, post_gain, w_query, w_key, w_value, w_out_t):
    old_start = offsets(old_blocks)
    new_start = offsets(new_blocks)
    seq_rows = jnp.arange(TOKENS, dtype=jnp.int32)
    shard = (lax.optimization_barrier(jnp.sum((old_start[None, :] <= seq_rows[:, None]).astype(jnp.int32), axis=1)) - 1).astype(jnp.int32)
    devices = jnp.arange(N_SEQ, dtype=jnp.int32)
    holder = lax.optimization_barrier(jnp.sum(devices[None, :] * (order[None, :] == shard[:, None]).astype(jnp.int32), axis=1)).astype(jnp.int32)
    source = (holder * CAP + seq_rows - old_start[shard]).astype(jnp.int32)
    resident = x_old[source]
    resident_f = resident.astype(jnp.float32)
    normed = rms_scale(resident_f, pre_gain).astype(jnp.bfloat16)
    query = jnp.dot(normed, w_query, preferred_element_type=jnp.float32).reshape(TOKENS, HEADS, HEAD)
    query = (rotate(query, seq_rows) * (D // HEADS) ** (-0.5)).astype(jnp.bfloat16)
    key = jnp.dot(normed, w_key, preferred_element_type=jnp.float32).reshape(TOKENS, KV_HEADS, HEAD)
    key = rotate(key, seq_rows).astype(jnp.bfloat16)
    value = jnp.dot(normed, w_value, preferred_element_type=jnp.float32).reshape(TOKENS, KV_HEADS, HEAD).astype(jnp.bfloat16)
    group = HEADS // KV_HEADS
    query_heads = jnp.transpose(query, (1, 0, 2)).astype(jnp.float32)
    key_heads = jnp.repeat(jnp.transpose(key, (1, 0, 2)), group, axis=0).astype(jnp.float32)
    value_heads = jnp.repeat(jnp.transpose(value, (1, 0, 2)), group, axis=0).astype(jnp.float32)
    causal = seq_rows[None, :] <= seq_rows[:, None]

    def one_head(operands):
        query_one, key_one, value_one = operands
        score = jnp.dot(query_one, key_one.T)
        capped = 50.0 * jnp.tanh(score / 50.0)
        weight = jnp.where(causal, jnp.exp(capped), 0.0)
        total = lax.optimization_barrier(jnp.sum(weight, axis=1))
        weight_b = weight.astype(jnp.bfloat16).astype(jnp.float32)
        numer = jnp.dot(weight_b, value_one)
        return (numer / total[:, None]).astype(jnp.bfloat16)
    context = lax.map(one_head, (query_heads, key_heads, value_heads))
    context = jnp.transpose(context, (1, 0, 2)).reshape(TOKENS, HEADS * HEAD)
    span = HEADS * HEAD // N_TP
    projected = jnp.zeros((TOKENS, D), jnp.float32)
    for group_index in range(N_TP):
        columns = context[:, group_index * span:(group_index + 1) * span]
        weights_part = w_out_t[:, group_index * span:(group_index + 1) * span]
        partial_sum = lax.dot_general(columns, weights_part, (((1,), (1,)), ((), ())), preferred_element_type=jnp.float32)
        projected = projected + lax.optimization_barrier(partial_sum.astype(jnp.bfloat16)).astype(jnp.float32)
    refreshed = (resident_f + rms_scale(projected, post_gain)).astype(jnp.bfloat16)
    slots = jnp.arange(N_SEQ * CAP, dtype=jnp.int32)
    owner = (slots // CAP).astype(jnp.int32)
    within = (slots - owner * CAP).astype(jnp.int32)
    valid = within < new_blocks[owner] * BLOCK
    target = jnp.clip(new_start[owner] + within, 0, TOKENS - 1).astype(jnp.int32)
    return jnp.where(valid[:, None], refreshed[target], jnp.zeros((), jnp.bfloat16)).astype(jnp.bfloat16)
```

```python
import functools
import math

import jax
import jax.numpy as jnp
from jax import lax
from jax.experimental import pallas as pl
from jax.experimental.pallas import tpu as pltpu
from jax.sharding import PartitionSpec as P

HEAD = 128
BLOCK = 128
EPS = 1e-06


def offsets(blocks):
    return (jnp.cumsum(blocks) - blocks) * BLOCK


def rms_scale(values, gain):
    return values * lax.rsqrt(jnp.mean(values * values, axis=-1, keepdims=True) + EPS) * gain


def attention_kernel(rows, span, q_ref, k_ref, v_ref, out_ref):
    first = pl.program_id(0) * rows
    query = q_ref[...]

    def step(at, carry, masked):
        numer, denom = carry
        start = pl.multiple_of(at * span, span)
        score = lax.dot_general(
            query,
            k_ref[pl.ds(start, span), :],
            (((1,), (1,)), ((), ())),
            preferred_element_type=jnp.float32,
        )
        weight = jnp.exp(50.0 * jnp.tanh(score * (1.0 / 50.0)))
        if masked:
            places = first + lax.broadcasted_iota(jnp.int32, weight.shape, 0)
            keys = start + lax.broadcasted_iota(jnp.int32, weight.shape, 1)
            weight = jnp.where(keys <= places, weight, 0.0)
        denom = denom + jnp.sum(weight, axis=1, keepdims=True)
        numer = numer + jnp.dot(
            weight.astype(jnp.bfloat16),
            v_ref[pl.ds(start, span), :],
            preferred_element_type=jnp.float32,
        )
        return numer, denom

    whole = first // span
    state = (jnp.zeros((rows, HEAD), jnp.float32), jnp.zeros((rows, 1), jnp.float32))
    state = lax.fori_loop(0, whole, lambda at, c: step(at, c, False), state)
    numer, denom = step(whole, state, True)
    out_ref[...] = (numer / denom).astype(out_ref.dtype)


def attention(query, key, value):
    tokens = query.shape[0]
    rows, span = 256, 512
    return pl.pallas_call(
        functools.partial(attention_kernel, rows, span),
        grid=(tokens // rows,),
        in_specs=[
            pl.BlockSpec((rows, HEAD), lambda i: (i, 0)),
            pl.BlockSpec((tokens, HEAD), lambda i: (0, 0)),
            pl.BlockSpec((tokens, HEAD), lambda i: (0, 0)),
        ],
        out_specs=pl.BlockSpec((rows, HEAD), lambda i: (i, 0)),
        out_shape=jax.ShapeDtypeStruct((tokens, HEAD), jnp.bfloat16),
        cost_estimate=pl.CostEstimate(
            flops=3 * tokens * tokens * HEAD,
            bytes_accessed=8 * tokens * HEAD,
            transcendentals=tokens * tokens,
        ),
    )(query, key, value)


def per_device(
    x_old, old_blocks, new_blocks, order, pre_gain, post_gain, w_query, w_key, w_value, w_out_t
):
    seq_count = lax.axis_size("seq")
    tp_count = lax.axis_size("tp")
    capacity, quarter = x_old.shape
    width = quarter * tp_count
    tokens = seq_count * capacity // 2
    own = tokens // seq_count
    share = capacity // tp_count
    seq_index = lax.axis_index("seq")
    tp_index = lax.axis_index("tp")
    old_start = offsets(old_blocks)
    new_start = offsets(new_blocks)
    device_ids = jnp.arange(seq_count, dtype=jnp.int32)

    gathered = lax.all_gather(x_old, "seq", axis=0, tiled=True)

    def stored(row, count):
        row = jnp.minimum(row, tokens - count)
        shard = jnp.sum((old_start <= row).astype(jnp.int32)) - 1
        holder = jnp.sum(jnp.where(order == shard, device_ids, 0))
        begin = jnp.sum(jnp.where(device_ids == shard, old_start, 0))
        return lax.dynamic_slice_in_dim(gathered, holder * capacity + row - begin, count, 0)

    def shift(k):
        return [(i, (i + k) % tp_count) for i in range(tp_count)]

    def by_source(received):
        stack = jnp.stack(received)
        pieces = [
            lax.dynamic_index_in_dim(stack, lax.rem(tp_index - u + tp_count, tp_count), 0, False)
            for u in range(tp_count)
        ]
        return jnp.concatenate(pieces, axis=1)

    mine = jnp.concatenate(
        [stored(seq_index * own + at, BLOCK) for at in range(0, own, BLOCK)], axis=0
    )
    full_rows = by_source(
        [mine] + [lax.ppermute(mine, "tp", shift(k)) for k in range(1, tp_count)]
    )
    my_start = jnp.sum(jnp.where(device_ids == seq_index, new_start, 0))
    my_count = jnp.sum(jnp.where(device_ids == seq_index, new_blocks, 0)) * BLOCK

    def slot_rows(place):
        return stored(my_start + place * share, share)

    residual = by_source(
        [slot_rows(tp_index)]
        + [
            lax.ppermute(slot_rows(lax.rem(tp_index + k, tp_count)), "tp", shift(k))
            for k in range(1, tp_count)
        ]
    ).astype(jnp.float32)

    weights = lax.all_gather(
        jnp.concatenate([w_query, w_key, w_value], axis=1), "seq", axis=0, tiled=True
    )
    out_full = lax.all_gather(w_out_t, "seq", axis=0, tiled=True)

    normed = rms_scale(full_rows.astype(jnp.float32), pre_gain).astype(jnp.bfloat16)
    heads = w_query.shape[1] // HEAD
    kv_heads = w_key.shape[1] // HEAD
    group = heads // kv_heads
    copies = seq_count // heads
    raw = jnp.dot(normed, weights, preferred_element_type=jnp.float32)

    half = HEAD // 2
    inverse = jnp.exp(jnp.arange(half, dtype=jnp.float32) * (-2.0 * math.log(10000.0) / HEAD))
    places = seq_index * own + jnp.arange(own, dtype=jnp.int32)
    angles = places.astype(jnp.float32)[:, None] * inverse[None, :]
    cosine, sine = jnp.cos(angles), jnp.sin(angles)

    def rotate(at):
        first = raw[:, at * HEAD : at * HEAD + half]
        second = raw[:, at * HEAD + half : (at + 1) * HEAD]
        return jnp.concatenate(
            [first * cosine - second * sine, second * cosine + first * sine], axis=-1
        )

    scale = (width // (heads * tp_count)) ** (-0.5)
    queries = [(rotate(h) * scale).astype(jnp.bfloat16) for h in range(heads)]
    keys = [rotate(heads + g).astype(jnp.bfloat16) for g in range(kv_heads)]
    values = [
        raw[:, (heads + kv_heads + g) * HEAD : (heads + kv_heads + g + 1) * HEAD].astype(
            jnp.bfloat16
        )
        for g in range(kv_heads)
    ]
    sent = jnp.stack(
        [
            jnp.stack([queries[s // copies], keys[s // copies // group], values[s // copies // group]])
            for s in range(seq_count)
        ]
    )
    came = lax.all_to_all(sent, "seq", 0, 0, tiled=True)
    context = attention(
        came[:, 0].reshape(tokens, HEAD),
        came[:, 1].reshape(tokens, HEAD),
        came[:, 2].reshape(tokens, HEAD),
    )
    padded = jnp.concatenate([context, jnp.zeros((capacity, HEAD), jnp.bfloat16)], axis=0)
    back = jnp.stack(
        [lax.dynamic_slice_in_dim(padded, new_start[j], capacity, 0) for j in range(seq_count)]
    )
    ours = lax.all_to_all(back, "seq", 0, 0, tiled=True)[::copies]
    ours = ours.reshape(heads, tp_count, share, HEAD)

    def partial(place):
        rows = lax.dynamic_index_in_dim(ours, place, 1, False)
        rows = jnp.transpose(rows, (1, 0, 2)).reshape(share, heads * HEAD)
        return lax.dot_general(
            rows, out_full, (((1,), (1,)), ((), ())), preferred_element_type=jnp.float32
        ).astype(jnp.bfloat16)

    pieces = [partial(lax.rem(tp_index + k, tp_count)) for k in range(tp_count)]
    right, left = None, None
    for k in range(1, tp_count):
        going_right = pieces[tp_count - k]
        going_left = pieces[k]
        if k > 1:
            going_right = (
                going_right.astype(jnp.float32) + right.astype(jnp.float32)
            ).astype(jnp.bfloat16)
            going_left = (
                going_left.astype(jnp.float32) + left.astype(jnp.float32)
            ).astype(jnp.bfloat16)
        right = lax.ppermute(going_right, "tp", [(i, i + 1) for i in range(k)])
        left = lax.ppermute(
            going_left, "tp", [(i, i - 1) for i in range(tp_count - k, tp_count)]
        )
    projected = (
        pieces[0].astype(jnp.float32) + right.astype(jnp.float32) + left.astype(jnp.float32)
    )
    refreshed = residual + rms_scale(projected, post_gain)
    live = tp_index * share + jnp.arange(share, dtype=jnp.int32) < my_count
    return jnp.where(live[:, None], refreshed, 0.0).astype(jnp.bfloat16)


def solution(mesh):
    placed = (
        P("seq", "tp"),
        P(),
        P(),
        P(),
        P(),
        P(),
        P("seq", "tp"),
        P("seq", "tp"),
        P("seq", "tp"),
        P("seq", "tp"),
    )
    return jax.shard_map(
        per_device, mesh=mesh, in_specs=placed, out_specs=P(("seq", "tp"), None), check_vma=False
    )
```

```python
import functools
import math

import jax
import jax.numpy as jnp
from jax import lax
from jax.experimental import pallas as pl
from jax.experimental.pallas import tpu as pltpu
from jax.sharding import PartitionSpec as P

HEAD = 128
BLOCK = 128
EPS = 1e-06


def offsets(blocks):
    return (jnp.cumsum(blocks) - blocks) * BLOCK


def rms_scale(values, gain):
    return values * lax.rsqrt(jnp.mean(values * values, axis=-1, keepdims=True) + EPS) * gain


def attention_kernel(rows, span, q_ref, k_ref, v_ref, out_ref):
    first = pl.program_id(0) * rows
    query = q_ref[...]

    def step(at, carry, masked):
        numer, denom = carry
        start = pl.multiple_of(at * span, span)
        score = lax.dot_general(
            query,
            k_ref[pl.ds(start, span), :],
            (((1,), (1,)), ((), ())),
            preferred_element_type=jnp.float32,
        )
        weight = jnp.exp(50.0 * jnp.tanh(score * (1.0 / 50.0)))
        if masked:
            places = first + lax.broadcasted_iota(jnp.int32, weight.shape, 0)
            keys = start + lax.broadcasted_iota(jnp.int32, weight.shape, 1)
            weight = jnp.where(keys <= places, weight, 0.0)
        denom = denom + jnp.sum(weight, axis=1, keepdims=True)
        numer = numer + jnp.dot(
            weight.astype(jnp.bfloat16),
            v_ref[pl.ds(start, span), :],
            preferred_element_type=jnp.float32,
        )
        return numer, denom

    whole = first // span
    state = (jnp.zeros((rows, HEAD), jnp.float32), jnp.zeros((rows, 1), jnp.float32))
    state = lax.fori_loop(0, whole, lambda at, c: step(at, c, False), state)
    numer, denom = step(whole, state, True)
    out_ref[...] = (numer / denom).astype(out_ref.dtype)


def attention(query, key, value):
    tokens = query.shape[0]
    rows, span = 256, 512
    return pl.pallas_call(
        functools.partial(attention_kernel, rows, span),
        grid=(tokens // rows,),
        in_specs=[
            pl.BlockSpec((rows, HEAD), lambda i: (i, 0)),
            pl.BlockSpec((tokens, HEAD), lambda i: (0, 0)),
            pl.BlockSpec((tokens, HEAD), lambda i: (0, 0)),
        ],
        out_specs=pl.BlockSpec((rows, HEAD), lambda i: (i, 0)),
        out_shape=jax.ShapeDtypeStruct((tokens, HEAD), jnp.bfloat16),
        cost_estimate=pl.CostEstimate(
            flops=3 * tokens * tokens * HEAD,
            bytes_accessed=8 * tokens * HEAD,
            transcendentals=tokens * tokens,
        ),
    )(query, key, value)


def per_device(
    x_old, old_blocks, new_blocks, order, pre_gain, post_gain, w_query, w_key, w_value, w_out_t
):
    seq_count = lax.axis_size("seq")
    tp_count = lax.axis_size("tp")
    capacity, quarter = x_old.shape
    width = quarter * tp_count
    tokens = seq_count * capacity // 2
    own = tokens // seq_count
    share = capacity // tp_count
    seq_index = lax.axis_index("seq")
    tp_index = lax.axis_index("tp")
    old_start = offsets(old_blocks)
    new_start = offsets(new_blocks)
    device_ids = jnp.arange(seq_count, dtype=jnp.int32)

    gathered = lax.all_gather(x_old, "seq", axis=0, tiled=True)

    def stored(row, count):
        row = jnp.minimum(row, tokens - count)
        shard = jnp.sum((old_start <= row).astype(jnp.int32)) - 1
        holder = jnp.sum(jnp.where(order == shard, device_ids, 0))
        begin = jnp.sum(jnp.where(device_ids == shard, old_start, 0))
        return lax.dynamic_slice_in_dim(gathered, holder * capacity + row - begin, count, 0)

    def shift(k):
        return [(i, (i + k) % tp_count) for i in range(tp_count)]

    def by_source(received):
        stack = jnp.stack(received)
        pieces = [
            lax.dynamic_index_in_dim(stack, lax.rem(tp_index - u + tp_count, tp_count), 0, False)
            for u in range(tp_count)
        ]
        return jnp.concatenate(pieces, axis=1)

    mine = jnp.concatenate(
        [stored(seq_index * own + at, BLOCK) for at in range(0, own, BLOCK)], axis=0
    )
    full_rows = by_source(
        [mine] + [lax.ppermute(mine, "tp", shift(k)) for k in range(1, tp_count)]
    )
    my_start = jnp.sum(jnp.where(device_ids == seq_index, new_start, 0))
    my_count = jnp.sum(jnp.where(device_ids == seq_index, new_blocks, 0)) * BLOCK

    def slot_rows(place):
        return stored(my_start + place * share, share)

    residual = by_source(
        [slot_rows(tp_index)]
        + [
            lax.ppermute(slot_rows(lax.rem(tp_index + k, tp_count)), "tp", shift(k))
            for k in range(1, tp_count)
        ]
    )

    weights = lax.all_gather(
        jnp.concatenate([w_query, w_key, w_value], axis=1), "seq", axis=0, tiled=True
    )
    out_full = lax.all_gather(w_out_t, "seq", axis=0, tiled=True)

    normed = rms_scale(full_rows.astype(jnp.float32), pre_gain).astype(jnp.bfloat16)
    normed, residual = lax.optimization_barrier((normed, residual))
    heads = w_query.shape[1] // HEAD
    kv_heads = w_key.shape[1] // HEAD
    group = heads // kv_heads
    copies = seq_count // heads
    raw = jnp.dot(normed, weights, preferred_element_type=jnp.float32)

    half = HEAD // 2
    inverse = jnp.exp(jnp.arange(half, dtype=jnp.float32) * (-2.0 * math.log(10000.0) / HEAD))
    places = seq_index * own + jnp.arange(own, dtype=jnp.int32)
    angles = places.astype(jnp.float32)[:, None] * inverse[None, :]
    cosine, sine = jnp.cos(angles), jnp.sin(angles)

    def rotate(at):
        first = raw[:, at * HEAD : at * HEAD + half]
        second = raw[:, at * HEAD + half : (at + 1) * HEAD]
        return jnp.concatenate(
            [first * cosine - second * sine, second * cosine + first * sine], axis=-1
        )

    scale = (width // (heads * tp_count)) ** (-0.5)
    queries = [(rotate(h) * scale).astype(jnp.bfloat16) for h in range(heads)]
    keys = [rotate(heads + g).astype(jnp.bfloat16) for g in range(kv_heads)]
    values = [
        raw[:, (heads + kv_heads + g) * HEAD : (heads + kv_heads + g + 1) * HEAD].astype(
            jnp.bfloat16
        )
        for g in range(kv_heads)
    ]
    sent = jnp.stack(
        [
            jnp.stack([queries[s // copies], keys[s // copies // group], values[s // copies // group]])
            for s in range(seq_count)
        ]
    )
    came = lax.all_to_all(sent, "seq", 0, 0, tiled=True)
    context = attention(
        came[:, 0].reshape(tokens, HEAD),
        came[:, 1].reshape(tokens, HEAD),
        came[:, 2].reshape(tokens, HEAD),
    )
    padded = jnp.concatenate([context, jnp.zeros((capacity, HEAD), jnp.bfloat16)], axis=0)
    back = jnp.stack(
        [lax.dynamic_slice_in_dim(padded, new_start[j], capacity, 0) for j in range(seq_count)]
    )
    ours = lax.all_to_all(back, "seq", 0, 0, tiled=True)[::copies]
    ours = ours.reshape(heads, tp_count, share, HEAD)

    def partial(place):
        rows = lax.dynamic_index_in_dim(ours, place, 1, False)
        rows = jnp.transpose(rows, (1, 0, 2)).reshape(share, heads * HEAD)
        return lax.dot_general(
            rows, out_full, (((1,), (1,)), ((), ())), preferred_element_type=jnp.float32
        ).astype(jnp.bfloat16)

    pieces = [partial(lax.rem(tp_index + k, tp_count)) for k in range(tp_count)]
    right, left = None, None
    for k in range(1, tp_count):
        going_right = pieces[tp_count - k]
        going_left = pieces[k]
        if k > 1:
            going_right = (
                going_right.astype(jnp.float32) + right.astype(jnp.float32)
            ).astype(jnp.bfloat16)
            going_left = (
                going_left.astype(jnp.float32) + left.astype(jnp.float32)
            ).astype(jnp.bfloat16)
        right = lax.ppermute(going_right, "tp", [(i, i + 1) for i in range(k)])
        left = lax.ppermute(
            going_left, "tp", [(i, i - 1) for i in range(tp_count - k, tp_count)]
        )
    projected = (
        pieces[0].astype(jnp.float32) + right.astype(jnp.float32) + left.astype(jnp.float32)
    )
    refreshed = residual.astype(jnp.float32) + rms_scale(projected, post_gain)
    live = tp_index * share + jnp.arange(share, dtype=jnp.int32) < my_count
    return jnp.where(live[:, None], refreshed, 0.0).astype(jnp.bfloat16)


def solution(mesh):
    placed = (
        P("seq", "tp"),
        P(),
        P(),
        P(),
        P(),
        P(),
        P("seq", "tp"),
        P("seq", "tp"),
        P("seq", "tp"),
        P("seq", "tp"),
    )
    return jax.shard_map(
        per_device, mesh=mesh, in_specs=placed, out_specs=P(("seq", "tp"), None), check_vma=False
    )
```

```python
import functools
import math

import jax
import jax.numpy as jnp
from jax import lax
from jax.experimental import pallas as pl
from jax.experimental.pallas import tpu as pltpu
from jax.sharding import PartitionSpec as P

HEAD = 128
BLOCK = 128
EPS = 1e-06


def offsets(blocks):
    return (jnp.cumsum(blocks) - blocks) * BLOCK


def rms_scale(values, gain):
    return values * lax.rsqrt(jnp.mean(values * values, axis=-1, keepdims=True) + EPS) * gain


def attention_kernel(rows, span, q_ref, k_ref, v_ref, out_ref):
    first = pl.program_id(0) * rows
    query = q_ref[...]

    def step(at, carry, masked):
        numer, denom = carry
        start = pl.multiple_of(at * span, span)
        score = lax.dot_general(
            query,
            k_ref[pl.ds(start, span), :],
            (((1,), (1,)), ((), ())),
            preferred_element_type=jnp.float32,
        )
        weight = jnp.exp(50.0 * jnp.tanh(score * (1.0 / 50.0)))
        if masked:
            places = first + lax.broadcasted_iota(jnp.int32, weight.shape, 0)
            keys = start + lax.broadcasted_iota(jnp.int32, weight.shape, 1)
            weight = jnp.where(keys <= places, weight, 0.0)
        denom = denom + jnp.sum(weight, axis=1, keepdims=True)
        numer = numer + jnp.dot(
            weight.astype(jnp.bfloat16),
            v_ref[pl.ds(start, span), :],
            preferred_element_type=jnp.float32,
        )
        return numer, denom

    whole = first // span
    state = (jnp.zeros((rows, HEAD), jnp.float32), jnp.zeros((rows, 1), jnp.float32))
    state = lax.fori_loop(0, whole, lambda at, c: step(at, c, False), state)
    numer, denom = step(whole, state, True)
    out_ref[...] = (numer / denom).astype(out_ref.dtype)


def attention(query, key, value):
    tokens = query.shape[0]
    rows, span = 256, 512
    return pl.pallas_call(
        functools.partial(attention_kernel, rows, span),
        grid=(tokens // rows,),
        in_specs=[
            pl.BlockSpec((rows, HEAD), lambda i: (i, 0)),
            pl.BlockSpec((tokens, HEAD), lambda i: (0, 0)),
            pl.BlockSpec((tokens, HEAD), lambda i: (0, 0)),
        ],
        out_specs=pl.BlockSpec((rows, HEAD), lambda i: (i, 0)),
        out_shape=jax.ShapeDtypeStruct((tokens, HEAD), jnp.bfloat16),
        cost_estimate=pl.CostEstimate(
            flops=3 * tokens * tokens * HEAD,
            bytes_accessed=8 * tokens * HEAD,
            transcendentals=tokens * tokens,
        ),
    )(query, key, value)


def per_device(
    x_old, old_blocks, new_blocks, order, pre_gain, post_gain, w_query, w_key, w_value, w_out_t
):
    seq_count = lax.axis_size("seq")
    tp_count = lax.axis_size("tp")
    capacity, quarter = x_old.shape
    width = quarter * tp_count
    tokens = seq_count * capacity // 2
    own = tokens // seq_count
    share = capacity // tp_count
    seq_index = lax.axis_index("seq")
    tp_index = lax.axis_index("tp")
    old_start = offsets(old_blocks)
    new_start = offsets(new_blocks)
    device_ids = jnp.arange(seq_count, dtype=jnp.int32)

    gathered = lax.all_gather(x_old, "seq", axis=0, tiled=True)

    def stored(row, count):
        row = jnp.minimum(row, tokens - count)
        shard = jnp.sum((old_start <= row).astype(jnp.int32)) - 1
        holder = jnp.sum(jnp.where(order == shard, device_ids, 0))
        begin = jnp.sum(jnp.where(device_ids == shard, old_start, 0))
        return lax.dynamic_slice_in_dim(gathered, holder * capacity + row - begin, count, 0)

    def shift(k):
        return [(i, (i + k) % tp_count) for i in range(tp_count)]

    def by_source(received):
        stack = jnp.stack(received)
        pieces = [
            lax.dynamic_index_in_dim(stack, lax.rem(tp_index - u + tp_count, tp_count), 0, False)
            for u in range(tp_count)
        ]
        return jnp.concatenate(pieces, axis=1)

    mine = jnp.concatenate(
        [stored(seq_index * own + at, BLOCK) for at in range(0, own, BLOCK)], axis=0
    )
    full_rows = by_source(
        [mine] + [lax.ppermute(mine, "tp", shift(k)) for k in range(1, tp_count)]
    )
    my_start = jnp.sum(jnp.where(device_ids == seq_index, new_start, 0))
    my_count = jnp.sum(jnp.where(device_ids == seq_index, new_blocks, 0)) * BLOCK

    def slot_rows(place):
        return stored(my_start + place * share, share)

    residual = by_source(
        [slot_rows(tp_index)]
        + [
            lax.ppermute(slot_rows(lax.rem(tp_index + k, tp_count)), "tp", shift(k))
            for k in range(1, tp_count)
        ]
    )

    weights = lax.all_gather(
        jnp.concatenate([w_query, w_key, w_value], axis=1), "seq", axis=0, tiled=True
    )
    out_full = lax.all_gather(w_out_t, "seq", axis=0, tiled=True)

    normed = rms_scale(full_rows.astype(jnp.float32), pre_gain).astype(jnp.bfloat16)
    normed, residual = lax.optimization_barrier((normed, residual))
    heads = w_query.shape[1] // HEAD
    kv_heads = w_key.shape[1] // HEAD
    group = heads // kv_heads
    copies = seq_count // heads
    raw = jnp.dot(normed, weights, preferred_element_type=jnp.float32)

    half = HEAD // 2
    inverse = jnp.exp(jnp.arange(half, dtype=jnp.float32) * (-2.0 * math.log(10000.0) / HEAD))
    places = seq_index * own + jnp.arange(own, dtype=jnp.int32)
    angles = places.astype(jnp.float32)[:, None] * inverse[None, :]
    cosine, sine = jnp.cos(angles), jnp.sin(angles)

    def rotate(at):
        first = raw[:, at * HEAD : at * HEAD + half]
        second = raw[:, at * HEAD + half : (at + 1) * HEAD]
        return jnp.concatenate(
            [first * cosine - second * sine, second * cosine + first * sine], axis=-1
        )

    scale = (width // (heads * tp_count)) ** (-0.5)
    queries = [(rotate(h) * scale).astype(jnp.bfloat16) for h in range(heads)]
    keys = [rotate(heads + g).astype(jnp.bfloat16) for g in range(kv_heads)]
    values = [
        raw[:, (heads + kv_heads + g) * HEAD : (heads + kv_heads + g + 1) * HEAD].astype(
            jnp.bfloat16
        )
        for g in range(kv_heads)
    ]
    sent = jnp.stack(
        [
            jnp.stack([queries[s // copies], keys[s // copies // group], values[s // copies // group]])
            for s in range(seq_count)
        ]
    )
    came = lax.all_to_all(sent, "seq", 0, 0, tiled=True)
    context = attention(
        came[:, 0].reshape(tokens, HEAD),
        came[:, 1].reshape(tokens, HEAD),
        came[:, 2].reshape(tokens, HEAD),
    )
    padded = jnp.concatenate([context, jnp.zeros((capacity, HEAD), jnp.bfloat16)], axis=0)
    back = jnp.stack(
        [lax.dynamic_slice_in_dim(padded, new_start[j], capacity, 0) for j in range(seq_count)]
    )
    ours = lax.all_to_all(back, "seq", 0, 0, tiled=True)[::copies]
    ours = ours.reshape(heads, tp_count, share, HEAD)

    def partials(steps):
        rows = jnp.stack(
            [
                lax.dynamic_index_in_dim(ours, lax.rem(tp_index + k, tp_count), 1, False)
                for k in steps
            ]
        )
        rows = jnp.transpose(rows, (0, 2, 1, 3)).reshape(len(steps) * share, heads * HEAD)
        product = lax.dot_general(
            rows, out_full, (((1,), (1,)), ((), ())), preferred_element_type=jnp.float32
        ).astype(jnp.bfloat16)
        return {k: product[at * share : (at + 1) * share] for at, k in enumerate(steps)}

    ends = [1, tp_count - 1]
    pieces = partials(ends) | partials([k for k in range(tp_count) if k not in ends])
    right, left = None, None
    for k in range(1, tp_count):
        going_right = pieces[tp_count - k]
        going_left = pieces[k]
        if k > 1:
            going_right = (
                going_right.astype(jnp.float32) + right.astype(jnp.float32)
            ).astype(jnp.bfloat16)
            going_left = (
                going_left.astype(jnp.float32) + left.astype(jnp.float32)
            ).astype(jnp.bfloat16)
        right = lax.ppermute(going_right, "tp", [(i, i + 1) for i in range(k)])
        left = lax.ppermute(
            going_left, "tp", [(i, i - 1) for i in range(tp_count - k, tp_count)]
        )
    projected = (
        pieces[0].astype(jnp.float32) + right.astype(jnp.float32) + left.astype(jnp.float32)
    )
    refreshed = residual.astype(jnp.float32) + rms_scale(projected, post_gain)
    live = tp_index * share + jnp.arange(share, dtype=jnp.int32) < my_count
    return jnp.where(live[:, None], refreshed, 0.0).astype(jnp.bfloat16)


def solution(mesh):
    placed = (
        P("seq", "tp"),
        P(),
        P(),
        P(),
        P(),
        P(),
        P("seq", "tp"),
        P("seq", "tp"),
        P("seq", "tp"),
        P("seq", "tp"),
    )
    return jax.shard_map(
        per_device, mesh=mesh, in_specs=placed, out_specs=P(("seq", "tp"), None), check_vma=False
    )
```
